32 devices in a mesh: row: 8 (over z, y), col: 4 (over x, core).
Axes of the slice: x: 2, y: 2, z: 4, core: 2. Of those that a mesh axis runs over, the one named last changes fastest.
Arguments:
- new_dosage: float32 [4096, 1024], P(('col', 'row')), may hold values from 0 to 2
- old_dosage: float32 [16384, 1024], P(('row', 'col')), may hold values from 0 to 2
- grm: bfloat16 [16384, 4096], P('row', 'col'), may hold values from -1.5 to 1.5
- counts: int32 [8], P('col'), may hold values from 256 to 512
- affected: int32 [32, 8], P('row', 'col'), may hold values from 0 to 1, as said below
Outputs:
- updated: bfloat16 [16384, 4096], P('row', 'col')
The draws below stay inside these ranges and needn't reach their ends.
Inputs may be any that keep to these rules, and one draw needn't show every extreme that they name: `affected`: the density of marked tile pairs differs from one tile of new samples to the next.
All inputs are finite; a program needn't handle non-finite values.
Results may differ from the reference program's by a relative error of at most 0.00115.
Values may be sent and summed in bfloat16 or wider, within the bound.
A program may use at most 128 MiB of HBM per device.

```python
import jax
import jax.numpy as jnp
from jax import lax

SNP = 1024
TILE = 512
REF_DEV = 2048
ALL = 16384
NEW = 4096
N_ROW = 8


def frequency_table(key):
    base_key, shift_key = jax.random.split(jax.random.fold_in(key, 5))
    base_rate = jax.random.uniform(base_key, (1, SNP), jnp.float32, 0.2, 0.8)
    shift_table = jax.random.uniform(shift_key, (16, SNP), jnp.float32, -0.15, 0.15)
    return base_rate + shift_table


def dosage_common(key, own_key, sample_count):
    frequency = frequency_table(key)
    subkeys = jax.random.split(own_key, 4)
    population = jax.random.randint(subkeys[0], (sample_count,), 0, 16)
    jitter = jax.random.uniform(subkeys[1], (sample_count, 1), jnp.float32, -0.02, 0.02)
    chance = jnp.clip(frequency[population] + jitter, 0.03, 0.97)
    allele_draw = jax.random.uniform(subkeys[2], (sample_count, SNP), jnp.float32, 0.0, 1.0)
    absent = (1.0 - chance) * (1.0 - chance)
    called = (allele_draw > absent).astype(jnp.float32) + (allele_draw > 1.0 - chance * chance).astype(jnp.float32)
    weight_draw = jax.random.uniform(subkeys[3], (sample_count, SNP), jnp.float32, 0.0, 1.0)
    shrinkage = 0.3 * weight_draw
    dosage = (1.0 - shrinkage) * called + shrinkage * 2.0 * chance
    return jnp.clip(dosage, 0.0, 2.0).astype(jnp.float32)


def draw_new_dosage(key, part):
    return dosage_common(key, jax.random.fold_in(key, 11), NEW)


def draw_old_dosage(key, part):
    return dosage_common(key, jax.random.fold_in(key, 23), ALL)


def draw_affected(key, part):
    first_key, second_key = jax.random.split(jax.random.fold_in(key, 37))
    offset = jax.random.randint(first_key, (), 0, 4)
    density = 1 + (jnp.arange(NEW // TILE) + offset) % 4
    tickets = jax.random.randint(second_key, (ALL // TILE, NEW // TILE), 0, 4)
    return (tickets < density[None, :]).astype(jnp.int32)


def touch_ends(drawn, key, least, top_value):
    dims = drawn.shape
    place = [jax.random.randint(jax.random.fold_in(key, axis), (), 0, dims[axis]) for axis in range(len(dims))]
    drawn = drawn.at[tuple(place)].set(least)
    longest = dims.index(max(dims))
    place[longest] = (place[longest] + 1) % dims[longest]
    return drawn.at[tuple(place)].set(top_value)


def level_of(key, shape, pieces, low, high):
    factor_of = 1.0
    for position, shards_of in pieces:
        draws = jax.random.uniform(jax.random.fold_in(jax.random.fold_in(key, 6), position), (shards_of,), jnp.float32, low / len(pieces), high / len(pieces))
        factor_of = factor_of * jnp.repeat(jnp.exp(draws), shape[position] // shards_of).reshape((-1,) + (1,) * (len(shape) - 1 - position))
    return factor_of


def gaussian(rng, shape, width, bound, cuts=(), held_as=jnp.bfloat16):
    values = width * jax.random.normal(rng, shape, jnp.float32)
    if cuts:
        values = values * level_of(rng, shape, cuts, -0.22, 0.18)
    return jnp.clip(values, -bound, bound).astype(held_as)


def setup_inputs(seed: int = 0) -> dict:
    arg_keys = jax.random.split(jax.random.key(seed), 6)
    new_dosage = draw_new_dosage(jax.random.fold_in(arg_keys[5], 71), 0)
    old_dosage = draw_old_dosage(jax.random.fold_in(arg_keys[5], 71), 0)
    grm = gaussian(arg_keys[2], (ALL, NEW), 0.1, 1.5, ((0, 8), (1, 4)))
    counts = touch_ends(jax.random.randint(arg_keys[3], (NEW // TILE,), TILE // 2, TILE + 1), jax.random.fold_in(arg_keys[3], 1), TILE // 2, TILE).astype(jnp.int32)
    affected = draw_affected(jax.random.fold_in(arg_keys[5], 71), 0)
    return {"new_dosage": new_dosage, "old_dosage": old_dosage, "grm": grm, "counts": counts, "affected": affected}


def reference(new_dosage, old_dosage, grm, counts, affected):
    totals = lax.optimization_barrier(jnp.sum(old_dosage, axis=0))
    doubled = totals / ALL
    spread = jnp.sqrt(doubled * (1.0 - 0.5 * doubled) + 0.1)
    usable = (jnp.arange(TILE)[None, :] < counts[:, None]).reshape(NEW).astype(jnp.float32)
    new_scores = ((new_dosage - doubled) / spread * usable[:, None]).astype(jnp.bfloat16)
    old_scores = ((old_dosage - doubled) / spread).astype(jnp.bfloat16)
    new_wide = new_scores.astype(jnp.float32)
    old_blocks = old_scores.reshape(N_ROW, REF_DEV, SNP)
    grm_blocks = grm.reshape(N_ROW, REF_DEV, NEW)
    mark_blocks = affected.reshape(N_ROW, REF_DEV // TILE, NEW // TILE)

    def update_block(operands):
        scores, grm_block, markers = operands
        product = jnp.dot(scores.astype(jnp.float32), new_wide.T, precision=lax.Precision.HIGHEST) / SNP
        spread_marks = jnp.repeat(jnp.repeat(markers.astype(jnp.float32), TILE, axis=0), TILE, axis=1)
        return (grm_block.astype(jnp.float32) + product * spread_marks).astype(jnp.bfloat16)
    updated = lax.map(update_block, (old_blocks, grm_blocks, mark_blocks))
    return updated.reshape(ALL, NEW)
```

```python
import functools

import jax
import jax.numpy as jnp
from jax import lax
from jax.experimental import pallas as pl
from jax.experimental.pallas import tpu as pltpu
from jax.sharding import PartitionSpec as P

MESH = pl.DeviceIdType.MESH
CORES = 2
OLD_CHUNKS = 4
NEW_CHUNKS = 2
FOLD = 128


def kernel(
    n_row, n_col, new_hbm, old_hbm, grm_hbm, counts_ref, affected_ref, out_ref,
    new_in, old_in, grm_in, new_buf, old_buf, part, part_row,
    load_sem, col_send, col_recv, row_send, row_recv,
    x_send, sib_send, old_recv, right_send, left_send, y_send, new_recv,
):
    snps = new_in.shape[1]
    new_rows, old_rows = new_in.shape[0], old_in.shape[0]
    out_rows, out_cols = out_ref.shape
    tile = out_cols // counts_ref.shape[0]
    minor = 1 << ((n_row.bit_length() - 1) // 2)
    major = n_row // minor
    chips = n_col // CORES
    old_chunk, new_chunk = old_rows // OLD_CHUNKS, new_rows // NEW_CHUNKS
    group = minor * new_rows
    folds = snps // FOLD

    row, col = lax.axis_index("row"), lax.axis_index("col")
    a, b = row // minor, row % minor
    chip, core = col // CORES, col % CORES
    sibling = chip * CORES + (CORES - 1 - core)

    old_load = pltpu.make_async_copy(old_hbm, old_in, load_sem.at[0])
    new_load = pltpu.make_async_copy(new_hbm, new_in, load_sem.at[1])
    grm_load = pltpu.make_async_copy(grm_hbm, grm_in, load_sem.at[2])
    old_load.start()
    new_load.start()

    barrier = pltpu.get_barrier_semaphore()
    for d in range(1, n_col):
        pl.semaphore_signal(barrier, inc=1, device_id=(row, (col + d) % n_col), device_id_type=MESH)
    for d in range(1, n_row):
        pl.semaphore_signal(barrier, inc=1, device_id=((row + d) % n_row, col), device_id_type=MESH)

    old_load.wait()
    grm_load.start()
    mine = jnp.sum(old_in[...], axis=0, keepdims=True)
    for f in range(folds):
        part[pl.ds(col, 1), f, :] = mine[:, f * FOLD:(f + 1) * FOLD]
    pl.semaphore_wait(barrier, n_col - 1 + n_row - 1)

    def exchange(buf, me, count, send, recv, target):
        for d in range(1, count):
            pltpu.make_async_remote_copy(
                buf.at[me], buf.at[me], send.at[d], recv.at[me],
                device_id=target((me + d) % count), device_id_type=MESH,
            ).start()
        for d in range(1, count):
            other = (me + d) % count
            pltpu.make_async_remote_copy(
                buf.at[other], buf.at[other], send.at[d], recv.at[other],
                device_id=target(other), device_id_type=MESH,
            ).wait()
        total = buf[0]
        for i in range(1, count):
            total = total + buf[i]
        return total

    col_total = exchange(part, col, n_col, col_send, col_recv, lambda i: (row, i))
    part_row[row] = col_total
    total = exchange(part_row, row, n_row, row_send, row_recv, lambda i: (i, col))
    totals = jnp.concatenate([total[f:f + 1] for f in range(folds)], axis=1)
    doubled = totals / (old_rows * n_row * n_col)
    inverse = 1.0 / jnp.sqrt(doubled * (1.0 - 0.5 * doubled) + 0.1)

    def ds(start, size, step):
        return pl.ds(pl.multiple_of(start, step), size)

    def old_part(j, k):
        return old_buf.at[ds(j * old_rows + k * old_chunk, old_chunk, old_chunk), :]

    def new_part(r, k):
        return new_buf.at[ds(r * new_rows + k * new_chunk, new_chunk, new_chunk), :]

    def old_copy(j, k, send, to):
        return pltpu.make_async_remote_copy(
            old_part(j, k), old_part(j, k), send, old_recv.at[j, k],
            device_id=(row, to), device_id_type=MESH,
        )

    def new_copy(r, k, send, to):
        return pltpu.make_async_remote_copy(
            new_part(r, k), new_part(r, k), send, new_recv.at[r, k],
            device_id=(to, col), device_id_type=MESH,
        )

    sends = []

    def start_if(cond, copy):
        @pl.when(cond)
        def _():
            copy.start()
        sends.append((cond, copy))

    def send_y(z, s, k):
        out = []
        for d in range(1, minor):
            out.append(new_copy(z * minor + b, k, y_send.at[s, d, k], a * minor + (b + d) % minor))
        return out

    new_load.wait()
    first = (row * new_rows) % tile
    count = counts_ref[(row * new_rows) // tile]
    for k in range(NEW_CHUNKS):
        place = lax.broadcasted_iota(jnp.int32, (new_chunk, 1), 0) + (first + k * new_chunk)
        usable = (place < count).astype(jnp.float32)
        rows = new_in[k * new_chunk:(k + 1) * new_chunk, :]
        new_buf[ds(row * new_rows + k * new_chunk, new_chunk, new_chunk), :] = (
            (rows - doubled) * inverse * usable
        ).astype(jnp.bfloat16)
        start_if(a < major - 1, new_copy(row, k, right_send.at[0, k], row + minor))
        start_if(a > 0, new_copy(row, k, left_send.at[0, k], row - minor))
        for copy in send_y(a, 0, k):
            copy.start()
            sends.append((None, copy))
    for k in range(OLD_CHUNKS):
        rows = old_in[k * old_chunk:(k + 1) * old_chunk, :]
        old_buf[ds(col * old_rows + k * old_chunk, old_chunk, old_chunk), :] = (
            (rows - doubled) * inverse
        ).astype(jnp.bfloat16)
        for d in range(1, chips):
            copy = old_copy(col, k, x_send.at[d, k], (chip + d) % chips * CORES + core)
            copy.start()
            sends.append((None, copy))
        copy = old_copy(col, k, sib_send.at[0, k], sibling)
        copy.start()
        sends.append((None, copy))

    grm_load.wait()

    def relay(s):
        for k in range(NEW_CHUNKS):
            for left in (True, False):
                z = a - 1 - s if left else a + 1 + s
                valid = z >= 0 if left else z < major
                onward = valid & (a < major - 1) if left else valid & (a > 0)
                r = z * minor + b
                dest = row + minor if left else row - minor
                send = right_send if left else left_send

                @pl.when(valid)
                def _():
                    new_copy(r, k, send.at[s + 1, k], row).wait_recv()
                start_if(onward, new_copy(r, k, send.at[s + 1, k], dest))
                slot = 1 + 2 * s + (0 if left else 1)
                for copy in send_y(z, slot, k):
                    start_if(valid, copy)

    def wait_y(z):
        for k in range(NEW_CHUNKS):
            for d in range(1, minor):
                r = z * minor + (b + d) % minor
                new_copy(r, k, y_send.at[0, d, k], row).wait_recv()

    def forward_old(k):
        for d in range(1, chips):
            j = (chip + d) % chips * CORES + core
            old_copy(j, k, sib_send.at[d, k], sibling).wait_recv()
            copy = old_copy(j, k, sib_send.at[d, k], sibling)
            copy.start()
            sends.append((None, copy))

    def wait_sib_own():
        for k in range(OLD_CHUNKS):
            old_copy(sibling, k, sib_send.at[0, k], sibling).wait_recv()

    def wait_sib_forwarded(k):
        for d in range(1, chips):
            j = (chip + d) % chips * CORES + (CORES - 1 - core)
            old_copy(j, k, sib_send.at[d, k], sibling).wait_recv()

    def block(z, start, size):
        cols = ds(z * group, group, group)
        rows = ds(start, size, size)
        mark = affected_ref[start // tile, (z * group) // tile].astype(jnp.float32)
        product = lax.dot_general(
            old_buf[rows, :], new_buf[cols, :], (((1,), (1,)), ((), ())),
            preferred_element_type=jnp.float32,
        )
        out_ref[rows, cols] = (
            grm_in[rows, cols].astype(jnp.float32) + product * (mark / snps)
        ).astype(jnp.bfloat16)

    def local_rows(z):
        size = min(256, old_rows)
        per = old_rows // size

        @pl.loop(0, CORES * per)
        def _(i):
            block(z, chip * CORES * old_rows + i * size, size)

    def far_rows(z, k, which):
        for d in range(1, chips):
            for c in which:
                j = (chip + d) % chips * CORES + c
                block(z, j * old_rows + k * old_chunk, old_chunk)

    both = (core, CORES - 1 - core)

    def far_loop(z, k0, k1):
        @pl.loop(k0, k1)
        def _(k):
            far_rows(z, k, both)

    def step_groups(s, body):
        for left in (True, False):
            z = a - 1 - s if left else a + 1 + s

            @pl.when(z >= 0 if left else z < major)
            def _():
                body(z)

    relay(0)
    forward_old(0)
    wait_sib_own()
    wait_y(a)
    local_rows(a)
    for s in range(1, major - 1):
        relay(s)
        if s < OLD_CHUNKS - 1:
            forward_old(s)
    for k in range(major - 1, OLD_CHUNKS - 1):
        forward_old(k)
    for k in range(OLD_CHUNKS - 1):
        wait_sib_forwarded(k)
    far_loop(a, 0, OLD_CHUNKS - 1)
    last = OLD_CHUNKS - 1

    def most(z):
        wait_y(z)
        local_rows(z)
        far_loop(z, 0, last)

    for s in range(major - 2):
        step_groups(s, most)
    forward_old(last)

    step_groups(major - 2, most)
    wait_sib_forwarded(last)

    @pl.loop(0, major)
    def _(z):
        far_rows(z, last, both)

    for cond, copy in sends:
        if cond is None:
            copy.wait_send()
        else:
            @pl.when(cond)
            def _():
                copy.wait_send()


def on_device(new_dosage, old_dosage, grm, counts, affected):
    n_row, n_col = lax.axis_size("row"), lax.axis_size("col")
    new_rows, snps = new_dosage.shape
    old_rows = old_dosage.shape[0]
    minor = 1 << ((n_row.bit_length() - 1) // 2)
    major = n_row // minor
    chips = n_col // CORES
    dma = pltpu.SemaphoreType.DMA
    hbm = pl.BlockSpec(memory_space=pltpu.HBM)
    smem = pl.BlockSpec(memory_space=pltpu.SMEM)
    return pl.pallas_call(
        functools.partial(kernel, n_row, n_col),
        out_shape=jax.ShapeDtypeStruct(grm.shape, grm.dtype),
        in_specs=[hbm, hbm, hbm, smem, smem],
        out_specs=pl.BlockSpec(memory_space=pltpu.VMEM),
        scratch_shapes=[
            pltpu.VMEM((new_rows, snps), jnp.float32),
            pltpu.VMEM((old_rows, snps), jnp.float32),
            pltpu.VMEM(grm.shape, grm.dtype),
            pltpu.VMEM((new_rows * n_row, snps), jnp.bfloat16),
            pltpu.VMEM((old_rows * n_col, snps), jnp.bfloat16),
            pltpu.VMEM((n_col, snps // FOLD, FOLD), jnp.float32),
            pltpu.VMEM((n_row, snps // FOLD, FOLD), jnp.float32),
            dma((3,)),
            dma((n_col,)),
            dma((n_col,)),
            dma((n_row,)),
            dma((n_row,)),
            dma((chips, OLD_CHUNKS)),
            dma((chips, OLD_CHUNKS)),
            dma((n_col, OLD_CHUNKS)),
            dma((major, NEW_CHUNKS)),
            dma((major, NEW_CHUNKS)),
            dma((2 * major, minor, NEW_CHUNKS)),
            dma((n_row, NEW_CHUNKS)),
        ],
        compiler_params=pltpu.CompilerParams(
            collective_id=0, has_side_effects=True, vmem_limit_bytes=40 * 1024 * 1024
        ),
    )(new_dosage, old_dosage, grm, counts, affected)


def solution(mesh):
    return jax.shard_map(
        on_device,
        mesh=mesh,
        in_specs=(
            P(("col", "row"), None),
            P(("row", "col"), None),
            P("row", "col"),
            P("col"),
            P("row", "col"),
        ),
        out_specs=P("row", "col"),
        check_vma=False,
    )
```

```python
import functools

import jax
import jax.numpy as jnp
from jax import lax
from jax.experimental import pallas as pl
from jax.experimental.pallas import tpu as pltpu
from jax.sharding import PartitionSpec as P

MESH = pl.DeviceIdType.MESH
CORES = 2
OLD_CHUNKS = 4
NEW_CHUNKS = 2
CODED = 2
FOLD = 128
LEVELS = 32767
STRIP = 32


def kernel(
    n_row, n_col, new_hbm, old_hbm, grm_hbm, counts_ref, affected_ref, out_ref,
    new_in, old_in, grm_in, new_code, old_code, new_buf, old_buf, part, part_row,
    load_sem, col_send, col_recv, row_send, row_recv,
    x_send, sib_send, old_recv, right_send, left_send, y_send, new_recv,
):
    snps = new_in.shape[1]
    new_rows, old_rows = new_in.shape[0], old_in.shape[0]
    out_rows, out_cols = out_ref.shape
    tile = out_cols // counts_ref.shape[0]
    minor = 1 << ((n_row.bit_length() - 1) // 2)
    major = n_row // minor
    chips = n_col // CORES
    old_chunk, new_chunk = old_rows // OLD_CHUNKS, new_rows // NEW_CHUNKS
    group = minor * new_rows
    folds = snps // FOLD

    row, col = lax.axis_index("row"), lax.axis_index("col")
    a, b = row // minor, row % minor
    chip, core = col // CORES, col % CORES
    sibling = chip * CORES + (CORES - 1 - core)

    old_load = pltpu.make_async_copy(old_hbm, old_in, load_sem.at[0])
    new_load = pltpu.make_async_copy(new_hbm, new_in, load_sem.at[1])
    grm_load = pltpu.make_async_copy(grm_hbm, grm_in, load_sem.at[2])
    old_load.start()
    new_load.start()

    barrier = pltpu.get_barrier_semaphore()
    for d in range(1, n_col):
        pl.semaphore_signal(barrier, inc=1, device_id=(row, (col + d) % n_col), device_id_type=MESH)
    for d in range(1, n_row):
        pl.semaphore_signal(barrier, inc=1, device_id=((row + d) % n_row, col), device_id_type=MESH)

    old_load.wait()
    grm_load.start()
    mine = jnp.sum(old_in[...], axis=0, keepdims=True)
    for f in range(folds):
        part[pl.ds(col, 1), f, :] = mine[:, f * FOLD:(f + 1) * FOLD]
    def ds(start, size, step):
        return pl.ds(pl.multiple_of(start, step), size)

    coded_rows = CODED * old_chunk

    def old_part(j, k):
        if k < CODED:
            return old_code.at[ds(j * coded_rows + k * old_chunk, old_chunk, old_chunk), :]
        return exact_part(j, k)

    def exact_part(j, k):
        return old_buf.at[ds(j * old_rows + k * old_chunk, old_chunk, old_chunk), :]

    def new_part(r, k):
        return new_code.at[ds(r * new_rows + k * new_chunk, new_chunk, new_chunk), :]

    def old_copy(j, k, send, to):
        return pltpu.make_async_remote_copy(
            old_part(j, k), old_part(j, k), send, old_recv.at[j, k],
            device_id=(row, to), device_id_type=MESH,
        )

    def own_copy(j, k):
        return pltpu.make_async_remote_copy(
            exact_part(j, k), exact_part(j, k), sib_send.at[0, k], old_recv.at[j, k],
            device_id=(row, sibling), device_id_type=MESH,
        )

    def new_copy(r, k, send, to):
        return pltpu.make_async_remote_copy(
            new_part(r, k), new_part(r, k), send, new_recv.at[r, k],
            device_id=(to, col), device_id_type=MESH,
        )

    sends = []

    def start(copy, cond=None):
        if cond is None:
            copy.start()
        else:
            @pl.when(cond)
            def _():
                copy.start()
        sends.append((cond, copy))

    def send_y(z, s, k):
        return [
            new_copy(z * minor + b, k, y_send.at[s, d, k], a * minor + (b + d) % minor)
            for d in range(1, minor)
        ]

    def encode(x):
        return ((x * LEVELS + 0.5).astype(jnp.int32) - LEVELS).astype(jnp.int16)

    new_load.wait()
    new_code[ds(row * new_rows, new_rows, new_rows), :] = encode(new_in[...])
    old_code[ds(col * coded_rows, coded_rows, coded_rows), :] = encode(old_in[:coded_rows, :])

    def send_new(k):
        start(new_copy(row, k, right_send.at[0, k], row + minor), a < major - 1)
        start(new_copy(row, k, left_send.at[0, k], row - minor), a > 0)
        for copy in send_y(a, 0, k):
            start(copy)

    def send_old(k):
        for d in range(1, chips):
            start(old_copy(col, k, x_send.at[d, k], (chip + d) % chips * CORES + core))

    def send_sums(buf, me, count, send, recv, target):
        for d in range(1, count):
            pltpu.make_async_remote_copy(
                buf.at[me], buf.at[me], send.at[d], recv.at[me],
                device_id=target((me + d) % count), device_id_type=MESH,
            ).start()

    def take_sums(buf, me, count, send, recv, target):
        for d in range(1, count):
            other = (me + d) % count
            pltpu.make_async_remote_copy(
                buf.at[other], buf.at[other], send.at[d], recv.at[other],
                device_id=target(other), device_id_type=MESH,
            ).wait()
        total = buf[0]
        for i in range(1, count):
            total = total + buf[i]
        return total

    over_col = (part, col, n_col, col_send, col_recv, lambda i: (row, i))
    over_row = (part_row, row, n_row, row_send, row_recv, lambda i: (i, col))

    pl.semaphore_wait(barrier, n_col - 1 + n_row - 1)
    send_sums(*over_col)
    send_new(0)
    for k in range(CODED):
        send_old(k)
    part_row[row] = take_sums(*over_col)
    send_sums(*over_row)
    for k in range(1, NEW_CHUNKS):
        send_new(k)

    def relay(s):
        for k in range(NEW_CHUNKS):
            for left in (True, False):
                z = a - 1 - s if left else a + 1 + s
                valid = z >= 0 if left else z < major
                onward = valid & (a < major - 1) if left else valid & (a > 0)
                r = z * minor + b
                dest = row + minor if left else row - minor
                send = right_send if left else left_send

                @pl.when(valid)
                def _():
                    new_copy(r, k, send.at[s + 1, k], row).wait_recv()
                start(new_copy(r, k, send.at[s + 1, k], dest), onward)
                slot = 1 + 2 * s + (0 if left else 1)
                for copy in send_y(z, slot, k):
                    start(copy, valid)

    def wait_y(z):
        for k in range(NEW_CHUNKS):
            for d in range(1, minor):
                r = z * minor + (b + d) % minor
                new_copy(r, k, y_send.at[0, d, k], row).wait_recv()

    def forward_old(k):
        for d in range(1, chips):
            j = (chip + d) % chips * CORES + core
            old_copy(j, k, sib_send.at[d, k], sibling).wait_recv()
            start(old_copy(j, k, sib_send.at[d, k], sibling))

    def wait_sib_own():
        for k in range(OLD_CHUNKS):
            own_copy(sibling, k).wait_recv()

    def wait_sib_forwarded(k):
        for d in range(1, chips):
            j = (chip + d) % chips * CORES + (CORES - 1 - core)
            old_copy(j, k, sib_send.at[d, k], sibling).wait_recv()

    def block(z, first, size):
        cols = ds(z * group, group, group)
        rows = ds(first, size, size)
        mark = affected_ref[(z * group) // tile, first // tile].astype(jnp.float32)
        product = lax.dot_general(
            old_buf[rows, :], new_buf[cols, :], (((1,), (1,)), ((), ())),
            preferred_element_type=jnp.float32,
        )
        out_ref[rows, cols] = (
            grm_in[rows, cols].astype(jnp.float32) + product * (mark / snps)
        ).astype(jnp.bfloat16)

    def local_rows(z):
        size = min(256, old_rows)
        per = old_rows // size

        @pl.loop(0, CORES * per)
        def _(i):
            block(z, chip * CORES * old_rows + i * size, size)

    def far_rows(z, k, which):
        for d in range(1, chips):
            for c in which:
                j = (chip + d) % chips * CORES + c
                block(z, j * old_rows + k * old_chunk, old_chunk)

    both = (core, CORES - 1 - core)

    def far_loop(z, k0, k1):
        @pl.loop(k0, k1)
        def _(k):
            far_rows(z, k, both)

    def step_groups(s, body):
        for left in (True, False):
            z = a - 1 - s if left else a + 1 + s

            @pl.when(z >= 0 if left else z < major)
            def _():
                body(z)

    relay(0)
    total = take_sums(*over_row)
    totals = jnp.concatenate([total[f:f + 1] for f in range(folds)], axis=1)
    doubled = totals / (old_rows * n_row * n_col)
    inverse = 1.0 / jnp.sqrt(doubled * (1.0 - 0.5 * doubled) + 0.1)
    code_scale = inverse / LEVELS
    code_shift = (1.0 - doubled) * inverse

    for k in reversed(range(OLD_CHUNKS)):
        rows = old_in[k * old_chunk:(k + 1) * old_chunk, :]
        old_buf[ds(col * old_rows + k * old_chunk, old_chunk, old_chunk), :] = (
            (rows - doubled) * inverse
        ).astype(jnp.bfloat16)
    for k in range(CODED, OLD_CHUNKS):
        send_old(k)
    for k in range(OLD_CHUNKS):
        start(own_copy(col, k))
    grm_load.wait()

    def decode(codes):
        return codes.astype(jnp.int32).astype(jnp.float32) * code_scale + code_shift

    def decode_new(z):
        count = counts_ref[(z * group) // tile]

        @pl.loop(0, group // STRIP)
        def _(i):
            at = z * group + i * STRIP
            place = lax.broadcasted_iota(jnp.int32, (STRIP, 1), 0) + at % tile
            usable = (place < count).astype(jnp.float32)
            rows = ds(at, STRIP, STRIP)
            new_buf[rows, :] = (decode(new_code[rows, :]) * usable).astype(jnp.bfloat16)

    def decode_old(k):
        if k >= CODED:
            return
        for d in range(1, chips):
            for c in both:
                j = (chip + d) % chips * CORES + c

                @pl.loop(0, old_chunk // STRIP)
                def _(i):
                    codes = old_code[ds(j * coded_rows + k * old_chunk + i * STRIP, STRIP, STRIP), :]
                    old_buf[ds(j * old_rows + k * old_chunk + i * STRIP, STRIP, STRIP), :] = (
                        decode(codes).astype(jnp.bfloat16)
                    )

    forward_old(0)
    wait_y(a)
    decode_new(a)
    wait_sib_own()
    local_rows(a)
    for s in range(1, major - 1):
        relay(s)
        if s < OLD_CHUNKS - 1:
            forward_old(s)
    for k in range(major - 1, OLD_CHUNKS - 1):
        forward_old(k)
    for k in range(OLD_CHUNKS - 1):
        wait_sib_forwarded(k)
        decode_old(k)
    far_loop(a, 0, OLD_CHUNKS - 1)
    last = OLD_CHUNKS - 1

    def most(z):
        wait_y(z)
        decode_new(z)
        local_rows(z)
        far_loop(z, 0, last)

    for s in range(major - 2):
        step_groups(s, most)
    forward_old(last)

    step_groups(major - 2, most)
    wait_sib_forwarded(last)

    @pl.loop(0, major)
    def _(z):
        far_rows(z, last, both)

    for cond, copy in sends:
        if cond is None:
            copy.wait_send()
        else:
            @pl.when(cond)
            def _():
                copy.wait_send()


def on_device(new_dosage, old_dosage, grm, counts, affected):
    n_row, n_col = lax.axis_size("row"), lax.axis_size("col")
    new_rows, snps = new_dosage.shape
    old_rows = old_dosage.shape[0]
    minor = 1 << ((n_row.bit_length() - 1) // 2)
    major = n_row // minor
    chips = n_col // CORES
    dma = pltpu.SemaphoreType.DMA
    hbm = pl.BlockSpec(memory_space=pltpu.HBM)
    smem = pl.BlockSpec(memory_space=pltpu.SMEM)
    return pl.pallas_call(
        functools.partial(kernel, n_row, n_col),
        out_shape=jax.ShapeDtypeStruct(grm.shape, grm.dtype),
        in_specs=[hbm, hbm, hbm, smem, smem],
        out_specs=pl.BlockSpec(memory_space=pltpu.VMEM),
        scratch_shapes=[
            pltpu.VMEM((new_rows, snps), jnp.float32),
            pltpu.VMEM((old_rows, snps), jnp.float32),
            pltpu.VMEM(grm.shape, grm.dtype),
            pltpu.VMEM((new_rows * n_row, snps), jnp.int16),
            pltpu.VMEM((old_rows // OLD_CHUNKS * CODED * n_col, snps), jnp.int16),
            pltpu.VMEM((new_rows * n_row, snps), jnp.bfloat16),
            pltpu.VMEM((old_rows * n_col, snps), jnp.bfloat16),
            pltpu.VMEM((n_col, snps // FOLD, FOLD), jnp.float32),
            pltpu.VMEM((n_row, snps // FOLD, FOLD), jnp.float32),
            dma((3,)),
            dma((n_col,)),
            dma((n_col,)),
            dma((n_row,)),
            dma((n_row,)),
            dma((chips, OLD_CHUNKS)),
            dma((chips, OLD_CHUNKS)),
            dma((n_col, OLD_CHUNKS)),
            dma((major, NEW_CHUNKS)),
            dma((major, NEW_CHUNKS)),
            dma((2 * major, minor, NEW_CHUNKS)),
            dma((n_row, NEW_CHUNKS)),
        ],
        compiler_params=pltpu.CompilerParams(
            collective_id=0, has_side_effects=True, vmem_limit_bytes=40 * 1024 * 1024
        ),
    )(new_dosage, old_dosage, grm, counts, affected.T)


def solution(mesh):
    return jax.shard_map(
        on_device,
        mesh=mesh,
        in_specs=(
            P(("col", "row"), None),
            P(("row", "col"), None),
            P("row", "col"),
            P("col"),
            P("row", "col"),
        ),
        out_specs=P("row", "col"),
        check_vma=False,
    )
```

```python
import functools

import jax
import jax.numpy as jnp
from jax import lax
from jax.experimental import pallas as pl
from jax.experimental.pallas import tpu as pltpu
from jax.sharding import PartitionSpec as P

MESH = pl.DeviceIdType.MESH
CORES = 2
OLD_CHUNKS = 4
NEW_CHUNKS = 2
CODED = 2
PAIR = 2
FOLD = 128
LEVELS = 32767
STRIP = 32


def kernel(
    n_row, n_col, new_hbm, old_hbm, grm_hbm, counts_ref, affected_ref, out_ref,
    new_in, old_in, grm_in, new_code, old_code, new_buf, old_buf, part, part_row,
    load_sem, col_send, col_recv, row_send, row_recv,
    x_send, sib_send, old_recv, right_send, left_send, y_send, new_recv,
):
    snps = new_in.shape[1]
    new_rows, old_rows = new_in.shape[0], old_in.shape[0]
    out_rows, out_cols = out_ref.shape
    tile = out_cols // counts_ref.shape[0]
    minor = 1 << ((n_row.bit_length() - 1) // 2)
    major = n_row // minor
    chips = n_col // CORES
    old_chunk, new_chunk = old_rows // OLD_CHUNKS, new_rows // NEW_CHUNKS
    group = minor * new_rows
    folds = snps // FOLD

    row, col = lax.axis_index("row"), lax.axis_index("col")
    a, b = row // minor, row % minor
    chip, core = col // CORES, col % CORES
    sibling = chip * CORES + (CORES - 1 - core)

    old_load = pltpu.make_async_copy(old_hbm, old_in, load_sem.at[0])
    new_load = pltpu.make_async_copy(new_hbm, new_in, load_sem.at[1])
    grm_load = pltpu.make_async_copy(grm_hbm, grm_in, load_sem.at[2])
    old_load.start()
    new_load.start()

    barrier = pltpu.get_barrier_semaphore()
    for d in range(1, n_col):
        pl.semaphore_signal(barrier, inc=1, device_id=(row, (col + d) % n_col), device_id_type=MESH)
    for d in range(1, n_row):
        pl.semaphore_signal(barrier, inc=1, device_id=((row + d) % n_row, col), device_id_type=MESH)

    old_load.wait()
    grm_load.start()
    mine = jnp.sum(old_in[...], axis=0, keepdims=True)
    for f in range(folds):
        part[pl.ds(col, 1), f, :] = mine[:, f * FOLD:(f + 1) * FOLD]
    def ds(start, size, step):
        return pl.ds(pl.multiple_of(start, step), size)

    def score_place(j, k):
        return ((j // CORES * OLD_CHUNKS + k) * CORES + j % CORES) * old_chunk

    def code_place(j, k):
        return ((j // CORES * CODED + k) * CORES + j % CORES) * old_chunk

    def old_part(j, k):
        if k < CODED:
            return old_code.at[ds(code_place(j, k), old_chunk, old_chunk), :]
        return exact_part(j, k)

    def exact_part(j, k):
        return old_buf.at[ds(score_place(j, k), old_chunk, old_chunk), :]

    def new_part(r, k):
        return new_code.at[ds(r * new_rows + k * new_chunk, new_chunk, new_chunk), :]

    def old_copy(j, k, send, to):
        return pltpu.make_async_remote_copy(
            old_part(j, k), old_part(j, k), send, old_recv.at[j, k],
            device_id=(row, to), device_id_type=MESH,
        )

    def own_copy(j, k):
        return pltpu.make_async_remote_copy(
            exact_part(j, k), exact_part(j, k), sib_send.at[0, k], old_recv.at[j, k],
            device_id=(row, sibling), device_id_type=MESH,
        )

    def new_copy(r, k, send, to):
        return pltpu.make_async_remote_copy(
            new_part(r, k), new_part(r, k), send, new_recv.at[r, k],
            device_id=(to, col), device_id_type=MESH,
        )

    sends = []

    def start(copy, cond=None):
        if cond is None:
            copy.start()
        else:
            @pl.when(cond)
            def _():
                copy.start()
        sends.append((cond, copy))

    def send_y(z, s, k):
        return [
            new_copy(z * minor + b, k, y_send.at[s, d, k], a * minor + (b + d) % minor)
            for d in range(1, minor)
        ]

    def encode(x):
        return ((x * LEVELS + 0.5).astype(jnp.int32) - LEVELS).astype(jnp.int16)

    new_load.wait()
    new_code[ds(row * new_rows, new_rows, new_rows), :] = encode(new_in[...])
    for k in range(CODED):
        old_code[ds(code_place(col, k), old_chunk, old_chunk), :] = encode(
            old_in[k * old_chunk:(k + 1) * old_chunk, :]
        )

    def send_new(k):
        start(new_copy(row, k, right_send.at[0, k], row + minor), a < major - 1)
        start(new_copy(row, k, left_send.at[0, k], row - minor), a > 0)
        for copy in send_y(a, 0, k):
            start(copy)

    def send_old(k):
        for d in range(1, chips):
            start(old_copy(col, k, x_send.at[d, k], (chip + d) % chips * CORES + core))

    def send_sums(buf, me, count, send, recv, target):
        for d in range(1, count):
            pltpu.make_async_remote_copy(
                buf.at[me], buf.at[me], send.at[d], recv.at[me],
                device_id=target((me + d) % count), device_id_type=MESH,
            ).start()

    def take_sums(buf, me, count, send, recv, target):
        for d in range(1, count):
            other = (me + d) % count
            pltpu.make_async_remote_copy(
                buf.at[other], buf.at[other], send.at[d], recv.at[other],
                device_id=target(other), device_id_type=MESH,
            ).wait()
        total = buf[0]
        for i in range(1, count):
            total = total + buf[i]
        return total

    over_col = (part, col, n_col, col_send, col_recv, lambda i: (row, i))
    over_row = (part_row, row, n_row, row_send, row_recv, lambda i: (i, col))

    pl.semaphore_wait(barrier, n_col - 1 + n_row - 1)
    send_sums(*over_col)
    send_new(0)
    for k in range(CODED):
        send_old(k)
    part_row[row] = take_sums(*over_col)
    send_sums(*over_row)
    for k in range(1, NEW_CHUNKS):
        send_new(k)

    def relay(s):
        for k in range(NEW_CHUNKS):
            for left in (True, False):
                z = a - 1 - s if left else a + 1 + s
                valid = z >= 0 if left else z < major
                onward = valid & (a < major - 1) if left else valid & (a > 0)
                r = z * minor + b
                dest = row + minor if left else row - minor
                send = right_send if left else left_send

                @pl.when(valid)
                def _():
                    new_copy(r, k, send.at[s + 1, k], row).wait_recv()
                start(new_copy(r, k, send.at[s + 1, k], dest), onward)
                slot = 1 + 2 * s + (0 if left else 1)
                for copy in send_y(z, slot, k):
                    start(copy, valid)

    def wait_y(z):
        for k in range(NEW_CHUNKS):
            for d in range(1, minor):
                r = z * minor + (b + d) % minor
                new_copy(r, k, y_send.at[0, d, k], row).wait_recv()

    def forward_old(k):
        for d in range(1, chips):
            j = (chip + d) % chips * CORES + core
            old_copy(j, k, sib_send.at[d, k], sibling).wait_recv()
            start(old_copy(j, k, sib_send.at[d, k], sibling))

    def wait_sib_own():
        for k in range(OLD_CHUNKS):
            own_copy(sibling, k).wait_recv()

    def wait_sib_forwarded(k):
        for d in range(1, chips):
            j = (chip + d) % chips * CORES + (CORES - 1 - core)
            old_copy(j, k, sib_send.at[d, k], sibling).wait_recv()

    def block(z, where, k0, count):
        cols = ds(z * group, group, group)
        unit = CORES * old_chunk
        product = lax.dot_general(
            old_buf[ds((where * OLD_CHUNKS + k0) * unit, count * unit, unit), :], new_buf[cols, :],
            (((1,), (1,)), ((), ())), preferred_element_type=jnp.float32,
        )
        for i in range(count):
            for c in range(CORES):
                first = (where * CORES + c) * old_rows + (k0 + i) * old_chunk
                rows = ds(first, old_chunk, old_chunk)
                mark = affected_ref[(z * group) // tile, first // tile].astype(jnp.float32)
                at = (i * CORES + c) * old_chunk
                out_ref[rows, cols] = (
                    grm_in[rows, cols].astype(jnp.float32)
                    + product[at:at + old_chunk, :] * (mark / snps)
                ).astype(jnp.bfloat16)

    def local_rows(z):
        @pl.loop(0, OLD_CHUNKS // PAIR)
        def _(i):
            block(z, chip, i * PAIR, PAIR)

    def far_rows(z, k0, count):
        for d in range(1, chips):
            block(z, (chip + d) % chips, k0, count)

    both = (core, CORES - 1 - core)

    def step_groups(s, body):
        for left in (True, False):
            z = a - 1 - s if left else a + 1 + s

            @pl.when(z >= 0 if left else z < major)
            def _():
                body(z)

    relay(0)
    total = take_sums(*over_row)
    totals = jnp.concatenate([total[f:f + 1] for f in range(folds)], axis=1)
    doubled = totals / (old_rows * n_row * n_col)
    inverse = 1.0 / jnp.sqrt(doubled * (1.0 - 0.5 * doubled) + 0.1)
    code_scale = inverse / LEVELS
    code_shift = (1.0 - doubled) * inverse

    for k in reversed(range(OLD_CHUNKS)):
        rows = old_in[k * old_chunk:(k + 1) * old_chunk, :]
        old_buf[ds(score_place(col, k), old_chunk, old_chunk), :] = (
            (rows - doubled) * inverse
        ).astype(jnp.bfloat16)
    for k in range(CODED, OLD_CHUNKS):
        send_old(k)
    for k in range(OLD_CHUNKS):
        start(own_copy(col, k))
    grm_load.wait()

    def decode(codes):
        return codes.astype(jnp.int32).astype(jnp.float32) * code_scale + code_shift

    def decode_new(z):
        count = counts_ref[(z * group) // tile]

        @pl.loop(0, group // STRIP)
        def _(i):
            at = z * group + i * STRIP
            place = lax.broadcasted_iota(jnp.int32, (STRIP, 1), 0) + at % tile
            usable = (place < count).astype(jnp.float32)
            rows = ds(at, STRIP, STRIP)
            new_buf[rows, :] = (decode(new_code[rows, :]) * usable).astype(jnp.bfloat16)

    def decode_old(k):
        if k >= CODED:
            return
        for d in range(1, chips):
            for c in both:
                j = (chip + d) % chips * CORES + c

                @pl.loop(0, old_chunk // STRIP)
                def _(i):
                    codes = old_code[ds(code_place(j, k) + i * STRIP, STRIP, STRIP), :]
                    old_buf[ds(score_place(j, k) + i * STRIP, STRIP, STRIP), :] = (
                        decode(codes).astype(jnp.bfloat16)
                    )

    forward_old(0)
    wait_y(a)
    decode_new(a)
    wait_sib_own()
    local_rows(a)
    for s in range(1, major - 1):
        relay(s)
        if s < OLD_CHUNKS - 1:
            forward_old(s)
    for k in range(major - 1, OLD_CHUNKS - 1):
        forward_old(k)
    for k in range(OLD_CHUNKS - 1):
        wait_sib_forwarded(k)
        decode_old(k)
    far_rows(a, 0, OLD_CHUNKS - 1)
    last = OLD_CHUNKS - 1

    def most(z):
        wait_y(z)
        decode_new(z)
        local_rows(z)
        far_rows(z, 0, last)

    for s in range(major - 2):
        step_groups(s, most)
    forward_old(last)

    step_groups(major - 2, most)
    wait_sib_forwarded(last)

    @pl.loop(0, major)
    def _(z):
        far_rows(z, last, 1)

    for cond, copy in sends:
        if cond is None:
            copy.wait_send()
        else:
            @pl.when(cond)
            def _():
                copy.wait_send()


def on_device(new_dosage, old_dosage, grm, counts, affected):
    n_row, n_col = lax.axis_size("row"), lax.axis_size("col")
    new_rows, snps = new_dosage.shape
    old_rows = old_dosage.shape[0]
    minor = 1 << ((n_row.bit_length() - 1) // 2)
    major = n_row // minor
    chips = n_col // CORES
    dma = pltpu.SemaphoreType.DMA
    hbm = pl.BlockSpec(memory_space=pltpu.HBM)
    smem = pl.BlockSpec(memory_space=pltpu.SMEM)
    return pl.pallas_call(
        functools.partial(kernel, n_row, n_col),
        out_shape=pltpu.VMEM(grm.shape, grm.dtype),
        in_specs=[hbm, hbm, hbm, smem, smem],
        out_specs=pl.BlockSpec(memory_space=pltpu.VMEM),
        scratch_shapes=[
            pltpu.VMEM((new_rows, snps), jnp.float32),
            pltpu.VMEM((old_rows, snps), jnp.float32),
            pltpu.VMEM(grm.shape, grm.dtype),
            pltpu.VMEM((new_rows * n_row, snps), jnp.int16),
            pltpu.VMEM((old_rows // OLD_CHUNKS * CODED * n_col, snps), jnp.int16),
            pltpu.VMEM((new_rows * n_row, snps), jnp.bfloat16),
            pltpu.VMEM((old_rows * n_col, snps), jnp.bfloat16),
            pltpu.VMEM((n_col, snps // FOLD, FOLD), jnp.float32),
            pltpu.VMEM((n_row, snps // FOLD, FOLD), jnp.float32),
            dma((3,)),
            dma((n_col,)),
            dma((n_col,)),
            dma((n_row,)),
            dma((n_row,)),
            dma((chips, OLD_CHUNKS)),
            dma((chips, OLD_CHUNKS)),
            dma((n_col, OLD_CHUNKS)),
            dma((major, NEW_CHUNKS)),
            dma((major, NEW_CHUNKS)),
            dma((2 * major, minor, NEW_CHUNKS)),
            dma((n_row, NEW_CHUNKS)),
        ],
        compiler_params=pltpu.CompilerParams(
            collective_id=0, has_side_effects=True, vmem_limit_bytes=56 * 1024 * 1024
        ),
    )(new_dosage, old_dosage, grm, counts, affected.T)


def solution(mesh):
    return jax.shard_map(
        on_device,
        mesh=mesh,
        in_specs=(
            P(("col", "row"), None),
            P(("row", "col"), None),
            P("row", "col"),
            P("col"),
            P("row", "col"),
        ),
        out_specs=P("row", "col"),
        check_vma=False,
    )
```
